64 devices in a mesh: data: 4 (over x, y), seq: 16 (over z, core).
Axes of the slice: x: 2, y: 2, z: 8, core: 2. Of those that a mesh axis runs over, the one named last changes fastest.
The devices are a block of a 4x4x8 slice.
Arguments:
- x_tok: bfloat16 [131072, 1024], P(('data', 'seq')), parts along dimension 0
- dy_tok: bfloat16 [131072, 1024], P(('data', 'seq')), parts along dimension 0
- ln_gamma: float32 [1024], replicated
- ln_beta: float32 [1024], replicated
- w_qkv: bfloat16 [1024, 3, 16, 64], replicated
- w_out: bfloat16 [1024, 1024], replicated
Outputs:
- output 1: bfloat16 [131072, 1024], P(('data', 'seq')), parts along dimension 0
- output 2: bfloat16 [131072, 1024], P(('data', 'seq')), parts along dimension 0
- output 3: float32 [4096, 3, 16, 64], P(('data', 'seq')), parts along dimension 0
- output 4: float32 [4096, 1024], P(('data', 'seq')), parts along dimension 0
- output 5: float32 [4096], P('data'), parts along dimension 0
- output 6: float32 [4096], P('data'), parts along dimension 0
There are 4 independent parts. The reference program is written for one: setup_inputs(seed, part) draws one part's arguments, and reference() takes and returns one part's arrays. A program takes and returns all parts, laid end to end along the dimension named above; an argument that names none is the same for every part.
All inputs are finite; a program needn't handle non-finite values.
Results may differ from the reference program's by a relative error of at most 0.00487299.
Values are sent between devices in bfloat16 or wider.
A program may use at most 768 MiB of HBM per device.

```python
import jax
import jax.numpy as jnp
from jax import lax

TOKENS_DEV = 2048
SEQ = 16
D = 1024
HEADS = 16
HEAD = D // HEADS
TOKENS = SEQ * TOKENS_DEV
LN_EPS = 1e-5


def setup_inputs(seed: int = 0, part: int = 0) -> dict:
    part_key = jax.random.fold_in(jax.random.key(seed), part)
    keys_part = jax.random.split(part_key, 5)
    keys_shared = jax.random.split(jax.random.key(seed + 1), 4)
    noise = jax.random.normal(keys_part[0], (SEQ, TOKENS_DEV, D), jnp.float32)
    shard_offs = jax.random.normal(keys_part[1], (SEQ, 1, D), jnp.float32)
    base_offs = 0.7 * jax.random.normal(keys_part[2], (1, 1, D), jnp.float32)
    x_tok = (noise + shard_offs + base_offs).reshape(TOKENS, D).astype(jnp.bfloat16)
    grad_mean = 0.5 * jax.random.normal(keys_part[3], (1, D), jnp.float32)
    dy_tok = (jax.random.normal(keys_part[4], (TOKENS, D), jnp.float32) + grad_mean).astype(jnp.bfloat16)
    ln_gamma = 1.0 + 0.3 * jax.random.normal(keys_shared[0], (D,), jnp.float32)
    ln_beta = 0.5 * jax.random.normal(keys_shared[1], (D,), jnp.float32)
    w_qkv = (jax.random.normal(keys_shared[2], (D, 3, HEADS, HEAD), jnp.float32) * D ** -0.5).astype(jnp.bfloat16)
    w_out = (jax.random.normal(keys_shared[3], (D, D), jnp.float32) * D ** -0.5).astype(jnp.bfloat16)
    return {"x_tok": x_tok, "dy_tok": dy_tok, "ln_gamma": ln_gamma, "ln_beta": ln_beta, "w_qkv": w_qkv, "w_out": w_out}


def phi_act(t):
    return jnp.where(t > 0, t + 1.0, jnp.exp(jnp.minimum(t, 0.0)))


def phi_slope(t):
    return jnp.where(t > 0, 1.0, jnp.exp(jnp.minimum(t, 0.0)))


def reference(x_tok, dy_tok, ln_gamma, ln_beta, w_qkv, w_out):
    x_f32 = x_tok.astype(jnp.float32)
    centered = x_f32 - jnp.mean(x_f32, axis=-1, keepdims=True)
    inv_std = lax.rsqrt(jnp.mean(centered * centered, axis=-1, keepdims=True) + LN_EPS)
    x_hat = centered * inv_std
    normed = (x_hat * ln_gamma + ln_beta).astype(jnp.bfloat16)
    w_flat = w_qkv.reshape(D, 3 * D)
    qkv_all = jnp.dot(normed, w_flat, preferred_element_type=jnp.float32).astype(jnp.bfloat16).reshape(TOKENS, 3, HEADS, HEAD)
    q_raw = qkv_all[:, 0].astype(jnp.float32)
    k_raw = qkv_all[:, 1].astype(jnp.float32)
    v_heads = qkv_all[:, 2].astype(jnp.float32)
    feat_q = phi_act(q_raw).astype(jnp.bfloat16).astype(jnp.float32)
    feat_k = phi_act(k_raw).astype(jnp.bfloat16).astype(jnp.float32)
    state_b = jnp.einsum("nhi,nhj->hij", feat_k, v_heads).astype(jnp.bfloat16).astype(jnp.float32)
    norm_b = jnp.sum(feat_k, axis=0).astype(jnp.bfloat16).astype(jnp.float32)
    numerator = jnp.einsum("nhi,hij->nhj", feat_q, state_b)
    denominator = jnp.einsum("nhi,hi->nh", feat_q, norm_b)
    att_f32 = numerator / denominator[:, :, None]
    att_out = att_f32.astype(jnp.bfloat16).reshape(TOKENS, D)
    y_tok = (x_f32 + jnp.dot(att_out, w_out, preferred_element_type=jnp.float32)).astype(jnp.bfloat16)
    dw_out = jnp.dot(att_out.T, dy_tok, preferred_element_type=jnp.float32)
    d_att = jnp.dot(dy_tok, w_out.T, preferred_element_type=jnp.float32).reshape(TOKENS, HEADS, HEAD)
    g_scaled = (d_att / denominator[:, :, None]).astype(jnp.bfloat16).astype(jnp.float32)
    correction = jnp.sum(g_scaled * att_f32, axis=-1)
    d_fq = jnp.einsum("nhj,hij->nhi", g_scaled, state_b) - correction[:, :, None] * norm_b
    d_state_b = jnp.einsum("nhi,nhj->hij", feat_q, g_scaled).astype(jnp.bfloat16).astype(jnp.float32)
    d_norm = -jnp.einsum("nh,nhi->hi", correction, feat_q)
    d_fk = jnp.einsum("nhj,hij->nhi", v_heads, d_state_b) + d_norm
    d_val = jnp.einsum("nhi,hij->nhj", feat_k, d_state_b)
    d_q = (d_fq * phi_slope(q_raw)).astype(jnp.bfloat16)
    d_k = (d_fk * phi_slope(k_raw)).astype(jnp.bfloat16)
    d_qkv = jnp.stack([d_q, d_k, d_val.astype(jnp.bfloat16)], axis=1).reshape(TOKENS, 3 * D)
    dw_qkv = jnp.dot(normed.T, d_qkv, preferred_element_type=jnp.float32).reshape(D, 3, HEADS, HEAD)
    d_normed = jnp.dot(d_qkv, w_flat.T, preferred_element_type=jnp.float32)
    d_gamma = jnp.sum(d_normed * x_hat, axis=0)
    d_beta = jnp.sum(d_normed, axis=0)
    scaled_grad = d_normed * ln_gamma
    d_ln = inv_std * (scaled_grad - jnp.mean(scaled_grad, axis=-1, keepdims=True) - x_hat * jnp.mean(scaled_grad * x_hat, axis=-1, keepdims=True))
    dx_tok = (dy_tok.astype(jnp.float32) + d_ln).astype(jnp.bfloat16)
    return (y_tok, dx_tok, dw_qkv, dw_out, d_gamma, d_beta)
```

```python
import functools

import jax
import jax.numpy as jnp
from jax import lax
from jax.experimental import pallas as pl
from jax.experimental.pallas import tpu as pltpu
from jax.sharding import PartitionSpec as P

LN_EPS = 1e-5
MESH = pl.DeviceIdType.MESH
BF = jnp.bfloat16
F32 = jnp.float32
TILE = 256
GROUP = 256
PIECE = 40
VMEM_LIMIT = 66 * 1024 * 1024 - 2 * 1024 * 1024 - 65536

NN = (((1,), (0,)), ((), ()))
NT = (((1,), (1,)), ((), ()))
TN = (((0,), (0,)), ((), ()))


def dot(a, b, dims=NN):
    return lax.dot_general(a, b, dims, preferred_element_type=F32)


def phi_act(t):
    return jnp.where(t > 0, t + 1.0, jnp.exp(jnp.minimum(t, 0.0)))


def phi_slope(t):
    return jnp.where(t > 0, 1.0, jnp.exp(jnp.minimum(t, 0.0)))


def cols(i, size):
    return pl.ds(pl.multiple_of(i * size, size), size)


class Where:
    def __init__(self, n):
        me = lax.axis_index("seq")
        self.chips = n // 2
        self.chip = me // 2
        self.core = lax.rem(me, 2)

    def at(self, offset):
        return {"seq": lax.rem(self.chip + offset + self.chips, self.chips) * 2 + self.core}

    def partner(self):
        return {"seq": self.chip * 2 + 1 - self.core}

    def source(self, offset):
        return lax.rem(self.chip + offset + self.chips, self.chips)

    def barrier(self):
        sem = pltpu.get_barrier_semaphore()
        for k in range(1, self.chips):
            pl.semaphore_signal(sem, inc=1, device_id=self.at(k), device_id_type=MESH)
        pl.semaphore_signal(sem, inc=1, device_id=self.partner(), device_id_type=MESH)
        pl.semaphore_wait(sem, self.chips)


def remote(src, dst, send, recv, device):
    return pltpu.make_async_remote_copy(
        src_ref=src, dst_ref=dst, send_sem=send, recv_sem=recv, device_id=device, device_id_type=MESH)


class StateSum:
    def __init__(self, w, part, pair, recv, fin, ssem, rsem):
        self.w, self.part, self.pair, self.recv, self.fin = w, part, pair, recv, fin
        self.ssem, self.rsem = ssem, rsem
        m = w.chips
        self.c0 = remote(part.at[1 - w.core], pair, ssem.at[0], rsem.at[0], w.partner())
        self.c1 = [remote(pair.at[w.source(k)], recv.at[k], ssem.at[k], rsem.at[k], w.at(k)) for k in range(1, m)]
        self.c2 = [
            remote(fin.at[w.core, w.chip], fin.at[w.core, w.chip], ssem.at[m + k], rsem.at[m + k], w.at(k))
            for k in range(1, m)]
        self.c3 = remote(fin.at[w.core], fin.at[w.core], ssem.at[m], rsem.at[m], w.partner())

    def start(self):
        self.c0.start()

    def exchange(self):
        w = self.w
        self.c0.wait()
        self.pair[...] = self.pair[...] + self.part[w.core]
        for c in self.c1:
            c.start()

    def own(self):
        w = self.w
        total = self.pair[w.chip]
        for k, c in enumerate(self.c1, 1):
            c.wait_recv()
            total = total + self.recv[k]
        self.fin[w.core, w.chip] = total
        for c in self.c2:
            c.start()

    def finish(self):
        for c in self.c2:
            c.wait_recv()
        self.c3.start()
        for c in self.c1 + self.c2:
            c.wait_send()
        self.c3.wait()


def put_state(part, g, state, vec):
    lane = lax.broadcasted_iota(jnp.int32, (64, 128), 1)
    for mm in range(2):
        block = state[128 * mm:128 * mm + 128, 128 * mm:128 * mm + 128]
        both = jnp.where(lane < 64, block[0:64], block[64:128])
        row = vec[:, 128 * mm:128 * mm + 128]
        for half in range(2):
            part[half, 2 * g + mm, 0:32, :] = both[32 * half:32 * half + 32]
            part[half, 2 * g + mm, 32:40, :] = row


def get_state(fin, m):
    both = jnp.concatenate([fin[0, m, 0:32, :], fin[1, m, 0:32, :]], axis=0)
    lane = lax.broadcasted_iota(jnp.int32, (64, 128), 1)
    block = jnp.concatenate([jnp.where(lane < 64, both, 0.0), jnp.where(lane < 64, 0.0, both)], axis=0)
    return block, fin[0, m, 32:40, :]


def spread(row):
    return jnp.transpose(jnp.concatenate([row] * 16, axis=0))


def norm_rows(x):
    x = x.astype(F32)
    centered = x - jnp.mean(x, axis=-1, keepdims=True)
    inv_std = lax.rsqrt(jnp.mean(centered * centered, axis=-1, keepdims=True) + LN_EPS)
    return centered * inv_std, inv_std


def front(n, x_hbm, dy_hbm, gamma_ref, beta_ref, wt_hbm, wo_hbm,
          ut_hbm, q_hbm, k_hbm, v_hbm, do_hbm, fin_out,
          x, dy, wt, wo, u, ut, q, k, v, do, part, pair, recv, fin, ssem, rsem, lsem, xsem, osem):
    w = Where(n)
    tokens, width = x.shape
    tiles, groups = tokens // TILE, width // GROUP
    state = StateSum(w, part, pair, recv, fin, ssem, rsem)

    def x_copy(t):
        return pltpu.make_async_copy(x_hbm.at[pl.ds(t * TILE, TILE)], x.at[pl.ds(t * TILE, TILE)], xsem.at[t])

    loads = [
        pltpu.make_async_copy(wt_hbm.at[pl.ds(width, 2 * width)], wt.at[pl.ds(width, 2 * width)], lsem.at[0]),
        pltpu.make_async_copy(wt_hbm.at[pl.ds(0, width)], wt.at[pl.ds(0, width)], lsem.at[1]),
        pltpu.make_async_copy(wo_hbm, wo, lsem.at[2]),
        pltpu.make_async_copy(dy_hbm, dy, lsem.at[3]),
    ]
    x_copy(0).start()
    loads[0].start()
    for t in range(1, tiles):
        x_copy(t).start()
    for c in loads[1:]:
        c.start()
    w.barrier()
    loads[0].wait()

    def kv_tile(t, carry):
        x_copy(t).wait()

        def rows(r, c):
            at = pl.ds(pl.multiple_of(r * 64, 64), 64)
            x_hat, _ = norm_rows(x[pl.ds(pl.multiple_of(t * TILE + r * 64, 64), 64), :])
            u[at, :] = (x_hat * gamma_ref[...] + beta_ref[...]).astype(BF)
            return c

        lax.fori_loop(0, TILE // 64, rows, 0)
        ut[:, cols(t, TILE)] = jnp.transpose(u[...])
        k[:, cols(t, TILE)] = dot(wt[width:2 * width], u[...], NT).astype(BF)
        v[:, cols(t, TILE)] = dot(wt[2 * width:3 * width], u[...], NT).astype(BF)
        return carry

    lax.fori_loop(0, tiles, kv_tile, 0)
    outs = [
        pltpu.make_async_copy(ut, ut_hbm, osem.at[0]),
        pltpu.make_async_copy(k, k_hbm, osem.at[1]),
        pltpu.make_async_copy(v, v_hbm, osem.at[2]),
        pltpu.make_async_copy(q, q_hbm, osem.at[3]),
        pltpu.make_async_copy(do, do_hbm, osem.at[4]),
    ]
    for c in outs[:3]:
        c.start()

    ones = jnp.ones((16, tokens), BF)
    for g in range(groups):
        at = slice(g * GROUP, (g + 1) * GROUP)
        fk = phi_act(k[at, :].astype(F32)).astype(BF)
        put_state(part, g, dot(fk, v[at, :], NT), dot(ones, fk, NT)[0:8])
    state.start()
    loads[1].wait()

    def q_tile(t, carry):
        q[:, cols(t, TILE)] = dot(wt[0:width], ut[:, cols(t, TILE)]).astype(BF)
        return carry

    def do_tile(t, carry):
        do[:, cols(t, TILE)] = dot(wo[...], dy[pl.ds(pl.multiple_of(t * TILE, TILE), TILE), :], NT)
        return carry

    early = tiles // 4
    lax.fori_loop(0, early, q_tile, 0)
    state.exchange()
    lax.fori_loop(early, tiles, q_tile, 0)
    outs[3].start()
    loads[2].wait()
    loads[3].wait()
    lax.fori_loop(0, early, do_tile, 0)
    state.own()
    lax.fori_loop(early, tiles, do_tile, 0)
    outs[4].start()
    state.finish()
    fin_out[...] = fin[...]
    for c in outs:
        c.wait()


class Ring:
    def __init__(self, w, blk, pair, recv, dssem, drsem, ssem, rsem, outs):
        self.w, self.blk, self.pair, self.recv = w, blk, pair, recv
        self.ssem, self.rsem, self.outs = ssem, rsem, outs
        self.d2d = [
            remote(blk.at[b % 2, :, 1 - w.core], pair.at[b], dssem.at[b], drsem.at[b], w.partner())
            for b in range(len(outs))]
        self.queue, self.pending, self.sent, self.freed = [], [], [], set()

    def copy(self, b, s, d):
        w, steps = self.w, self.w.chips - 1
        lanes = pl.ds(256 * d, 256)
        sem = (b * steps + s) * 2 + d
        to = w.at(1) if d == 0 else w.at(-1)
        if s == 0:
            src = self.pair.at[b, w.source(-1 if d == 0 else 1), :, lanes]
        else:
            src = self.recv.at[b, s - 1, d]
        return remote(src, self.recv.at[b, s, d], self.ssem.at[sem], self.rsem.at[sem], to)

    def free(self, b):
        if b >= 0 and b not in self.freed:
            while b in self.pending:
                self.join()
            self.d2d[b].wait_send()
            self.freed.add(b)

    def block(self, b):
        self.d2d[b].start()
        self.pending.append(b)

    def join(self):
        b = self.pending.pop(0)
        w = self.w
        self.d2d[b].wait_recv()
        for j in range(w.chips):
            self.pair[b, j] = self.pair[b, j] + self.blk[b % 2, j, w.core]
        for d in range(2):
            c = self.copy(b, 0, d)
            c.start()
            self.sent.append(c)
        self.queue.append((b, 0))

    def step(self):
        b, s = self.queue.pop(0)
        w, last = self.w, self.w.chips - 2
        for d in range(2):
            lanes = slice(256 * d, 256 * d + 256)
            self.copy(b, s, d).wait_recv()
            j = w.source(-2 - s if d == 0 else 2 + s) if s < last else w.chip
            total = self.recv[b, s, d] + self.pair[b, j, :, lanes]
            if s == last:
                out, first = self.outs[b]
                out[:, first + 256 * d:first + 256 * d + 256] = total
            else:
                self.recv[b, s, d] = total
                c = self.copy(b, s + 1, d)
                c.start()
                self.sent.append(c)
        if s < last:
            self.queue.append((b, s + 1))

    def tick(self, steps=2, fresh=0):
        while len(self.pending) > fresh:
            self.join()
        for _ in range(min(steps, len(self.queue))):
            self.step()

    def drain(self, blocks):
        while self.pending:
            self.join()
        while self.queue:
            self.step()
        for b in range(blocks):
            self.free(b)
        for c in self.sent:
            c.wait_send()


def back(n, x_hbm, dy_hbm, gamma_ref, beta_ref, wt_hbm, wo_hbm, ut_hbm, q_hbm, k_hbm, v_hbm, do_hbm, sfin,
         y_hbm, dx_hbm, dwq_out, dwo_out, dg_out, db_out,
         big, wo, ut, q, k, v, do, xt, dyt, ot, du, sbd, sbdt, zrow, zcol, rden, dzacc, gacc, bacc,
         part, pair, recv, fin, blk, rpair, rrecv, gb, gpair, gall,
         ssem, rsem, dssem, drsem, rssem, rrsem, gssem, grsem, lsem, qsem, dosem, xsem, dysem, osem):
    w = Where(n)
    width, tokens = q.shape
    half = tokens // 2
    tiles, groups = tokens // TILE, width // GROUP
    chunk = do.shape[2]
    chunks = tokens // chunk
    streams = width // 512

    def q_copy(i):
        return pltpu.make_async_copy(q_hbm.at[:, pl.ds(i * chunk, chunk)], q.at[:, pl.ds(i * chunk, chunk)], qsem.at[i])

    def do_copy(i):
        return pltpu.make_async_copy(do_hbm.at[:, pl.ds(i * chunk, chunk)], do.at[i % 2], dosem.at[i % 2])

    dy_loads = [pltpu.make_async_copy(dy_hbm.at[pl.ds(i * half, half)], big.at[2 + i], lsem.at[i]) for i in range(2)]
    ut_load = pltpu.make_async_copy(ut_hbm, ut, lsem.at[2])
    k_load = pltpu.make_async_copy(k_hbm, k, lsem.at[3])
    v_load = pltpu.make_async_copy(v_hbm, v, lsem.at[4])
    wo_load = pltpu.make_async_copy(wo_hbm, wo, lsem.at[5])
    wt_loads = [pltpu.make_async_copy(wt_hbm.at[pl.ds(i * width, width)], big.at[i], lsem.at[6 + i]) for i in range(3)]
    for i in range(chunks):
        q_copy(i).start()
    for c in dy_loads:
        c.start()
    do_copy(0).start()
    do_copy(1).start()
    for c in (ut_load, wo_load, k_load, v_load):
        c.start()
    w.barrier()

    outs = ([(dwo_out, 512 * i) for i in range(streams)]
            + [(dwq_out, 512 * i) for i in range(3 * streams)])
    ring = Ring(w, blk, rpair, rrecv, dssem, drsem, rssem, rrsem, outs)
    state = StateSum(w, part, pair, recv, fin, ssem, rsem)

    sbd[...] = jnp.zeros_like(sbd)
    sbdt[...] = jnp.zeros_like(sbdt)

    def build(source, with_rows):
        for m in range(w.chips):
            g, at = m // 2, slice(128 * (m % 2), 128 * (m % 2) + 128)
            block, row = get_state(source, m)
            sbd[g, at, at] = block.astype(BF)
            sbdt[g, at, at] = jnp.transpose(block).astype(BF)
            if with_rows:
                row = row.astype(BF).astype(F32)
                head = lax.broadcasted_iota(jnp.int32, (16, 128), 0) - 2 * (m % 2)
                lane = lax.broadcasted_iota(jnp.int32, (16, 128), 1) // 64
                zrow[g, :, at] = jnp.where(head == lane, jnp.concatenate([row, row], axis=0), 0.0).astype(BF)
            zcol[pl.ds(128 * m, 128), :] = spread(row)

    build(sfin, True)

    def attend(g, at):
        rows = cols(g, GROUP)
        qf = q[rows, at].astype(F32)
        fq = phi_act(qf).astype(BF)
        num = dot(sbdt[g], fq)
        return qf, fq, num

    for i in range(chunks):
        q_copy(i).wait()

        def o_group(g, carry, i=i):
            at = pl.ds(i * chunk, chunk)
            _, fq, num = attend(g, at)
            inv = 1.0 / dot(zrow[g], fq)[0:8]
            rden[g, :, at] = inv
            for r in range(4):
                a = num[64 * r:64 * r + 64] * inv[r:r + 1]
                first = i * chunk % half
                big[i * chunk // half, pl.ds(pl.multiple_of(g * GROUP + 64 * r, 64), 64), first:first + chunk] = a.astype(BF)
            return carry

        lax.fori_loop(0, groups, o_group, 0)

    for c in dy_loads:
        c.wait()

    def store_block(b, p, value):
        blk[b % 2, :, :, :, cols(p, 256)] = value.reshape(w.chips, 2, width // (2 * w.chips), 256)

    for i in range(streams):
        b = i
        ring.free(b - 2)

        def wo_part(p, carry, i=i, b=b):
            at = cols(2 * i + p, 256)
            store_block(b, p, dot(big[0], big[2, :, at]) + dot(big[1], big[3, :, at]))
            return carry

        lax.fori_loop(0, 2, wo_part, 0)
        ring.block(b)
        ring.tick(0, 1)

    dzacc[...] = jnp.zeros_like(dzacc)
    for i in range(chunks):
        do_copy(i).wait()

        def dq_group(g, carry, i=i):
            at = pl.ds(i * chunk, chunk)
            rows = cols(g, GROUP)
            qf, fq, num = attend(g, at)
            gs, cs = [], []
            for r in range(4):
                inv = rden[g, r:r + 1, at]
                a = num[64 * r:64 * r + 64] * inv
                gr = (do[i % 2, pl.ds(pl.multiple_of(g * GROUP + 64 * r, 64), 64), :] * inv).astype(BF)
                gs.append(gr)
                cs.append(jnp.sum(gr.astype(F32) * a, axis=0, keepdims=True))
            gg = jnp.concatenate(gs, axis=0)
            dfq = dot(sbd[g], gg)
            ds = dot(fq, gg, NT)
            at_g = cols(g, GROUP)
            du[:, at_g] = ds if i == 0 else du[:, at_g] + ds
            fqf = fq.astype(F32)
            for r in range(4):
                rr = slice(64 * r, 64 * r + 64)
                row = pl.ds(pl.multiple_of(g * GROUP + 64 * r, 64), 64)
                zc = zcol[row, :]
                total = dzacc[row, :]
                for j in range(chunk // 128):
                    lanes = slice(128 * j, 128 * j + 128)
                    c = cs[r][:, lanes]
                    qr = qf[rr, lanes]
                    dq = ((dfq[rr, lanes] - c * zc) * phi_slope(qr)).astype(BF)
                    q[row, pl.ds(i * chunk + 128 * j, 128)] = dq
                    total = total - c * fqf[rr, lanes]
                dzacc[row, :] = total
            return carry

        lax.fori_loop(0, groups, dq_group, 0)
        if i + 2 < chunks:
            do_copy(i + 2).start()
        ring.tick()

    for g in range(groups):
        rows = [jnp.sum(jnp.transpose(dzacc[pl.ds(g * GROUP + 128 * mm, 128), :]), axis=0, keepdims=True) for mm in range(2)]
        put_state(part, g, du[:, g * GROUP:(g + 1) * GROUP], jnp.broadcast_to(jnp.concatenate(rows, axis=1), (8, GROUP)))
    state.start()

    ut_load.wait()

    def grad_streams(first, d):
        for i in range(streams):
            b = first + i
            ring.free(b - 2)

            def part_of(p, carry, i=i, b=b):
                store_block(b, p, dot(ut[...], d[cols(2 * i + p, 256), :], NT))
                return carry

            lax.fori_loop(0, 2, part_of, 0)
            ring.block(b)
            if i == 0 and first == streams:
                state.exchange()
            ring.tick(fresh=1)

    grad_streams(streams, q)

    wo_load.wait()

    def x_copy(t, slot):
        return pltpu.make_async_copy(x_hbm.at[pl.ds(pl.multiple_of(t * TILE, TILE), TILE)], xt.at[slot], xsem.at[slot])

    def dy_copy(t, slot):
        return pltpu.make_async_copy(dy_hbm.at[pl.ds(pl.multiple_of(t * TILE, TILE), TILE)], dyt.at[slot], dysem.at[slot])

    def out_copy(hbm, t, slot):
        return pltpu.make_async_copy(ot.at[slot], hbm.at[pl.ds(pl.multiple_of(t * TILE, TILE), TILE)], osem.at[slot])

    x_copy(0, 0).start()
    for s in range(tiles // 2):
        def y_tile(t, carry):
            slot = lax.rem(t, 2)
            x_copy(t, slot).wait()

            @pl.when(t + 1 < tiles)
            def _():
                x_copy(t + 1, 1 - slot).start()

            @pl.when(t >= 2)
            def _():
                out_copy(y_hbm, t - 2, slot).wait()

            per = half // TILE
            at = cols(lax.rem(t, per), TILE)
            o = dot(big[lax.div(t, per), :, at], wo[...], TN)
            ot[slot] = (xt[slot].astype(F32) + o).astype(BF)
            out_copy(y_hbm, t, slot).start()
            return carry

        lax.fori_loop(2 * s, 2 * s + 2, y_tile, 0)
        if s == 0:
            state.own()
        ring.tick()
    out_copy(y_hbm, tiles - 2, 0).wait()
    out_copy(y_hbm, tiles - 1, 1).wait()
    for c in wt_loads:
        c.start()
    x_copy(0, 0).start()
    dy_copy(0, 0).start()
    state.finish()

    build(fin, False)
    k_load.wait()
    v_load.wait()
    for i in range(chunks):
        def dkv_group(g, carry, i=i):
            at = pl.ds(i * chunk, chunk)
            rows = cols(g, GROUP)
            kf = k[rows, at].astype(F32)
            fk = phi_act(kf).astype(BF)
            dv = dot(sbdt[g], fk).astype(BF)
            dfk = dot(sbd[g], v[rows, at])
            zc = zcol[rows, :]
            for j in range(chunk // 128):
                lanes = slice(128 * j, 128 * j + 128)
                k[rows, pl.ds(i * chunk + 128 * j, 128)] = ((dfk[:, lanes] + zc) * phi_slope(kf[:, lanes])).astype(BF)
            v[rows, at] = dv
            return carry

        lax.fori_loop(0, groups, dkv_group, 0)
        ring.tick()

    grad_streams(2 * streams, k)
    grad_streams(3 * streams, v)

    for c in wt_loads:
        c.wait()
    gacc[...] = jnp.zeros_like(gacc)
    bacc[...] = jnp.zeros_like(bacc)
    for s in range(tiles // 2):
        def dx_tile(t, carry):
            slot = lax.rem(t, 2)
            x_copy(t, slot).wait()
            dy_copy(t, slot).wait()

            @pl.when(t + 1 < tiles)
            def _():
                x_copy(t + 1, 1 - slot).start()
                dy_copy(t + 1, 1 - slot).start()

            @pl.when(t >= 2)
            def _():
                out_copy(dx_hbm, t - 2, slot).wait()

            at = cols(t, TILE)
            total = dot(q[:, at], big[0], TN) + dot(k[:, at], big[1], TN) + dot(v[:, at], big[2], TN)
            du[...] = total

            def rows(r, c):
                at = pl.ds(pl.multiple_of(r * 32, 32), 32)
                x_hat, inv_std = norm_rows(xt[slot, at, :])
                d = du[at, :]
                prod = d * x_hat
                gacc[...] += prod[0:8] + prod[8:16] + prod[16:24] + prod[24:32]
                bacc[...] += d[0:8] + d[8:16] + d[16:24] + d[24:32]
                e = d * gamma_ref[...]
                d_ln = inv_std * (e - jnp.mean(e, axis=-1, keepdims=True)
                                  - x_hat * jnp.mean(e * x_hat, axis=-1, keepdims=True))
                ot[slot, at, :] = (dyt[slot, at, :].astype(F32) + d_ln).astype(BF)
                return c

            lax.fori_loop(0, TILE // 32, rows, 0)
            out_copy(dx_hbm, t, slot).start()
            return carry

        lax.fori_loop(2 * s, 2 * s + 2, dx_tile, 0)
        ring.tick()

    gb[0] = gacc[...]
    gb[1] = bacc[...]
    swap = remote(gb, gpair, gssem.at[0], grsem.at[0], w.partner())
    swap.start()
    out_copy(dx_hbm, tiles - 2, 0).wait()
    out_copy(dx_hbm, tiles - 1, 1).wait()
    ring.tick()
    swap.wait()
    both = jnp.sum(gb[...] + gpair[...], axis=1, keepdims=True)
    gall[0] = jnp.broadcast_to(both, (2, 8, width))
    sends = [remote(gall.at[0], gall.at[j], gssem.at[j], grsem.at[j], w.at(j)) for j in range(1, w.chips)]
    for c in sends:
        c.start()
    ring.tick()
    ring.tick()
    for c in sends:
        c.wait()
    ring.drain(len(outs))
    total = gall[w.source(0)]
    for j in range(1, w.chips):
        total = total + gall[w.source(j)]
    dg_out[...] = total[0, 0:1]
    db_out[...] = total[1, 0:1]


def local_block(n, x_tok, dy_tok, ln_gamma, ln_beta, w_qkv, w_out):
    tokens, width = x_tok.shape
    chips = n // 2
    rows = width // n
    groups, tiles = width // GROUP, tokens // TILE
    chunk = min(512, tokens // 2)
    blocks = 4 * width // 512
    assert width // 128 == chips and w_qkv.shape[3] == 64
    wt = jnp.transpose(w_qkv, (1, 2, 3, 0)).reshape(3 * width, width)
    gamma, beta = ln_gamma.reshape(1, width), ln_beta.reshape(1, width)
    vmem, hbm = pl.BlockSpec(memory_space=pltpu.VMEM), pl.BlockSpec(memory_space=pl.ANY)
    dma = pltpu.SemaphoreType.DMA
    sums = [
        pltpu.VMEM((2, chips, PIECE, 128), F32),
        pltpu.VMEM((chips, PIECE, 128), F32),
        pltpu.VMEM((chips, PIECE, 128), F32),
        pltpu.VMEM((2, chips, PIECE, 128), F32),
    ]
    ut, q, k, v, do, fin = pl.pallas_call(
        functools.partial(front, n),
        name="front",
        out_shape=[jax.ShapeDtypeStruct((width, tokens), BF)] * 4
        + [jax.ShapeDtypeStruct((width, tokens), F32), jax.ShapeDtypeStruct((2, chips, PIECE, 128), F32)],
        in_specs=[hbm, hbm, vmem, vmem, hbm, hbm],
        out_specs=[hbm] * 5 + [vmem],
        scratch_shapes=[
            pltpu.VMEM((tokens, width), BF),
            pltpu.VMEM((tokens, width), BF),
            pltpu.VMEM((3 * width, width), BF),
            pltpu.VMEM((width, width), BF),
            pltpu.VMEM((TILE, width), BF),
            pltpu.VMEM((width, tokens), BF),
            pltpu.VMEM((width, tokens), BF),
            pltpu.VMEM((width, tokens), BF),
            pltpu.VMEM((width, tokens), BF),
            pltpu.VMEM((width, tokens), F32),
            *sums,
            dma((2 * chips,)), dma((2 * chips,)), dma((4,)), dma((tiles,)), dma((5,)),
        ],
        compiler_params=pltpu.CompilerParams(collective_id=0, has_side_effects=True, vmem_limit_bytes=VMEM_LIMIT),
    )(x_tok, dy_tok, gamma, beta, wt, w_out)
    steps = (chips - 1) * 2 * blocks
    y, dx, dwq, dwo, dg, db = pl.pallas_call(
        functools.partial(back, n),
        name="back",
        out_shape=[
            jax.ShapeDtypeStruct((tokens, width), BF),
            jax.ShapeDtypeStruct((tokens, width), BF),
            jax.ShapeDtypeStruct((rows, 3 * width), F32),
            jax.ShapeDtypeStruct((rows, width), F32),
            jax.ShapeDtypeStruct((1, width), F32),
            jax.ShapeDtypeStruct((1, width), F32),
        ],
        in_specs=[hbm, hbm, vmem, vmem, hbm, hbm, hbm, hbm, hbm, hbm, hbm, vmem],
        out_specs=[hbm, hbm, vmem, vmem, vmem, vmem],
        scratch_shapes=[
            pltpu.VMEM((4, width, tokens // 2), BF),
            pltpu.VMEM((width, width), BF),
            pltpu.VMEM((width, tokens), BF),
            pltpu.VMEM((width, tokens), BF),
            pltpu.VMEM((width, tokens), BF),
            pltpu.VMEM((width, tokens), BF),
            pltpu.VMEM((2, width, chunk), F32),
            pltpu.VMEM((2, TILE, width), BF),
            pltpu.VMEM((2, TILE, width), BF),
            pltpu.VMEM((2, TILE, width), BF),
            pltpu.VMEM((TILE, width), F32),
            pltpu.VMEM((groups, GROUP, GROUP), BF),
            pltpu.VMEM((groups, GROUP, GROUP), BF),
            pltpu.VMEM((groups, 16, GROUP), BF),
            pltpu.VMEM((width, 128), F32),
            pltpu.VMEM((groups, 8, tokens), F32),
            pltpu.VMEM((width, 128), F32),
            pltpu.VMEM((8, width), F32),
            pltpu.VMEM((8, width), F32),
            *sums,
            pltpu.VMEM((2, chips, 2, rows, 512), F32),
            pltpu.VMEM((blocks, chips, rows, 512), F32),
            pltpu.VMEM((blocks, chips - 1, 2, rows, 256), F32),
            pltpu.VMEM((2, 8, width), F32),
            pltpu.VMEM((2, 8, width), F32),
            pltpu.VMEM((chips, 2, 8, width), F32),
            dma((2 * chips,)), dma((2 * chips,)), dma((blocks,)), dma((blocks,)), dma((steps,)), dma((steps,)),
            dma((chips,)), dma((chips,)), dma((9,)), dma((tokens // chunk,)), dma((2,)), dma((2,)), dma((2,)), dma((2,)),
        ],
        compiler_params=pltpu.CompilerParams(collective_id=1, has_side_effects=True, vmem_limit_bytes=VMEM_LIMIT),
    )(x_tok, dy_tok, gamma, beta, wt, w_out, ut, q, k, v, do, fin)
    return (y, dx, dwq.reshape(rows, 3, w_qkv.shape[2], w_qkv.shape[3]), dwo, dg.reshape(width), db.reshape(width))


def solution(mesh):
    rows = P(("data", "seq"), None)
    return jax.shard_map(
        functools.partial(local_block, mesh.shape["seq"]), mesh=mesh,
        in_specs=(rows, rows, P(None), P(None), P(None, None, None, None), P(None, None)),
        out_specs=(rows, rows, P(("data", "seq"), None, None, None), rows, P("data"), P("data")),
        check_vma=False)
```
